32 devices in a mesh: ctx: 8 (over z, y), head: 4 (over x, core).
Axes of the slice: x: 2, y: 2, z: 4, core: 2. Of those that a mesh axis runs over, the one named last changes fastest.
Arguments:
- queries: bfloat16 [1024, 8192], P('ctx', 'head'), may hold values from -6 to 6
- key_rows: bfloat16 [1024, 1024], P(('ctx', 'head')), may hold values from -6 to 6
- value_matrix_rows: bfloat16 [1024, 1024], P(('ctx', 'head')), may hold values from -6 to 6
- grad_out: bfloat16 [1024, 8192], P('ctx', 'head'), may hold values from -6 to 6
- doc_ids: int32 [1024], replicated, may hold values from 0 to 3, never falling along the last dimension, each value on 1 to 512 neighbouring positions
- block_owner: int32 [8, 8], replicated, may hold values from 0 to 7, each once within a row
Outputs:
- attention: bfloat16 [1024, 8192], P('ctx', 'head')
- owned_lse: float32 [64, 1024], P('head', 'ctx')
- grad_query: bfloat16 [1024, 8192], P('ctx', 'head')
- key_gradient: bfloat16 [1024, 1024], P(('ctx', 'head'))
- value_gradient: bfloat16 [1024, 1024], P(('ctx', 'head'))
The draws below stay inside these ranges and needn't reach their ends.
Inputs may be any that keep to these rules, and one draw needn't show every extreme that they name: `doc_ids`: never falls along the tokens; every document holds 1 to 512 tokens. `block_owner`: entry [d, i] names the device that owns block i (tokens d * 128 + i * 16 onward, 16 of them) of token shard d; each row names every device once.
All inputs are finite; a program needn't handle non-finite values.
Results may differ from the reference program's by a relative error of at most 0.02.
Values may be sent and summed in bfloat16 or wider, within the bound.
No kernel may reach another device: no remote copies, remote signals or barrier semaphores. Data moves between devices by JAX's collectives and lax.ppermute only.
A program may use at most 64 MiB of HBM per device.

```python
import math
import jax
import jax.numpy as jnp
import numpy as np
from jax import lax

HQ = 64
KEY_VALUE_HEADS = 8
HEAD_SIZE = 128
DOCS = 4
QUERY_PER_KV = 8
SHARDS = 8
PACKED_TOKENS = 1024
BLK = 16
MOST_DOC = 512


def draw_queries(key, part):
    sampled_plan = jax.random.normal(jax.random.fold_in(key, 1), (PACKED_TOKENS, HQ * HEAD_SIZE), jnp.float32)
    return jnp.clip(sampled_plan, -6.0, 6.0).astype(jnp.bfloat16)


def draw_key_rows(key, part):
    sampled_plan = jax.random.normal(jax.random.fold_in(key, 3), (PACKED_TOKENS, KEY_VALUE_HEADS * HEAD_SIZE), jnp.float32)
    return jnp.clip(sampled_plan, -6.0, 6.0).astype(jnp.bfloat16)


def steps_of(stream_key, extent, pieces, low, high):
    level = 1.0
    for position, shards_of in pieces:
        heights = jax.random.uniform(jax.random.fold_in(jax.random.fold_in(stream_key, 6), position), (shards_of,), jnp.float32, low / len(pieces), high / len(pieces))
        level = level * jnp.repeat(jnp.exp(heights), extent[position] // shards_of).reshape((-1,) + (1,) * (len(extent) - 1 - position))
    return level


def profile(amount, total, most, skew):
    loads = [(1 << 20) // math.isqrt(grade ** skew) + 1 for grade in range(2, amount + 1)]
    spare, counts = total - most - (amount - 1), [1] * (amount - 1)
    while spare > 0:
        candidates = [i for i in range(amount - 1) if counts[i] < most]
        mass, remaining = sum([loads[i] for i in candidates]), spare
        for i in candidates:
            extra = min(most - counts[i], max(1, remaining * loads[i] // mass), spare)
            counts[i] = counts[i] + extra
            spare = spare - extra
    return np.array([most] + counts)


def uneven(stream_key, count, total, reach, skew):
    if count == 2:
        one = jax.random.randint(stream_key, (), max(1, total - reach), min(reach, total - 1) + 1)
        return jnp.stack([one, total - one])
    sizes = jnp.asarray(profile(count, total, reach, skew), jnp.int32)
    twos = (count - 1) // 2
    donor, sink = sizes[1:1 + 2 * twos:2], sizes[2:2 + 2 * twos:2]
    room = jnp.minimum(donor - 1, reach - sink)
    passed = jax.random.randint(jax.random.fold_in(stream_key, 1), (twos,), 0, 1 << 20) % (room + 1)
    sizes = sizes.at[1:1 + 2 * twos:2].set(donor - passed).at[2:2 + 2 * twos:2].set(sink + passed)
    return sizes[jax.random.permutation(jax.random.fold_in(stream_key, 2), count)]


def centred(own_key, dims, spread, reach, pieces=(), held_as=jnp.bfloat16):
    result = spread * jax.random.normal(own_key, dims, jnp.float32)
    if pieces:
        result = result * steps_of(own_key, dims, pieces, -0.22, 0.18)
    return jnp.clip(result, -reach, reach).astype(held_as)


def setup_inputs(seed: int = 0) -> dict:
    key_list = jax.random.split(jax.random.key(seed), 7)
    return {
        "queries": draw_queries(jax.random.fold_in(key_list[6], 71), 0),
        "key_rows": draw_key_rows(jax.random.fold_in(key_list[6], 71), 0),
        "value_matrix_rows": centred(key_list[2], (PACKED_TOKENS, KEY_VALUE_HEADS * HEAD_SIZE), 1.0, 6.0, ((0, 32),)),
        "grad_out": centred(key_list[3], (PACKED_TOKENS, HQ * HEAD_SIZE), 1.0, 6.0, ((0, 8), (1, 4))),
        "doc_ids": jnp.searchsorted(jnp.cumsum(uneven(key_list[4], DOCS, PACKED_TOKENS, MOST_DOC, 2)), jnp.arange(PACKED_TOKENS), side="right").astype(jnp.int32),
        "block_owner": jax.vmap(lambda own: jax.random.permutation(own, SHARDS))(jax.random.split(key_list[5], SHARDS)).reshape((SHARDS, SHARDS)).astype(jnp.int32),
    }


mask_value = -1.0e30


def reference(queries, key_rows, value_matrix_rows, grad_out, doc_ids, block_owner):
    score_scale = HEAD_SIZE ** -0.5
    positions = jnp.arange(PACKED_TOKENS, dtype=jnp.int32)
    allowed = (doc_ids[:, None] == doc_ids[None, :]) & (positions[None, :] <= positions[:, None])

    def per_head(head_index):
        group_index = head_index // QUERY_PER_KV
        query_head = lax.dynamic_slice_in_dim(queries, (head_index * HEAD_SIZE).astype(jnp.int32), HEAD_SIZE, 1)
        grad_head = lax.dynamic_slice_in_dim(grad_out, (head_index * HEAD_SIZE).astype(jnp.int32), HEAD_SIZE, 1)
        key_head = lax.dynamic_slice_in_dim(key_rows, (group_index * HEAD_SIZE).astype(jnp.int32), HEAD_SIZE, 1)
        value_head = lax.dynamic_slice_in_dim(value_matrix_rows, (group_index * HEAD_SIZE).astype(jnp.int32), HEAD_SIZE, 1)
        scores = jnp.dot(query_head, key_head.T, preferred_element_type=jnp.float32) * score_scale
        masked = jnp.where(allowed, scores, mask_value)
        row_max = jnp.max(masked, axis=1)
        weights_raw = jnp.where(allowed, jnp.exp(masked - row_max[:, None]), 0.0)
        row_sum = jnp.sum(weights_raw, axis=1)
        output_head = (jnp.dot(weights_raw.astype(jnp.bfloat16), value_head, preferred_element_type=jnp.float32) / row_sum[:, None]).astype(jnp.bfloat16)
        log_norm = row_max + jnp.log(row_sum)
        row_delta = jnp.sum(grad_head.astype(jnp.float32) * output_head.astype(jnp.float32), axis=1)
        probability = jnp.where(allowed, jnp.exp(masked - log_norm[:, None]), 0.0)
        dprob = jnp.dot(grad_head, value_head.T, preferred_element_type=jnp.float32)
        dscore = probability * (dprob - row_delta[:, None])
        dscore_low = dscore.astype(jnp.bfloat16)
        query_grad = (jnp.dot(dscore_low, key_head, preferred_element_type=jnp.float32) * score_scale).astype(jnp.bfloat16)
        key_grad = jnp.dot(dscore_low.T, query_head, preferred_element_type=jnp.float32) * score_scale
        value_grad = jnp.dot(probability.astype(jnp.bfloat16).T, grad_head, preferred_element_type=jnp.float32)
        return output_head, log_norm, query_grad, key_grad, value_grad

    result_list = lax.map(per_head, jnp.arange(HQ, dtype=jnp.int32))
    attention = result_list[0].transpose(1, 0, 2).reshape(PACKED_TOKENS, HQ * HEAD_SIZE)
    log_norm = result_list[1]
    grad_query = result_list[2].transpose(1, 0, 2).reshape(PACKED_TOKENS, HQ * HEAD_SIZE)
    key_gradient = result_list[3].reshape(KEY_VALUE_HEADS, QUERY_PER_KV, PACKED_TOKENS, HEAD_SIZE).sum(axis=1).transpose(1, 0, 2).reshape(PACKED_TOKENS, KEY_VALUE_HEADS * HEAD_SIZE).astype(jnp.bfloat16)
    value_gradient = result_list[4].reshape(KEY_VALUE_HEADS, QUERY_PER_KV, PACKED_TOKENS, HEAD_SIZE).sum(axis=1).transpose(1, 0, 2).reshape(PACKED_TOKENS, KEY_VALUE_HEADS * HEAD_SIZE).astype(jnp.bfloat16)
    inverse = jnp.argsort(block_owner, axis=1).astype(jnp.int32)
    split_lse = log_norm.reshape(HQ, SHARDS, SHARDS, BLK)
    gather_index = jnp.broadcast_to(inverse[None, :, :, None], split_lse.shape)
    picked = jnp.take_along_axis(split_lse, gather_index, axis=2)
    owned_lse = picked.transpose(0, 2, 1, 3).reshape(HQ, PACKED_TOKENS)
    return attention, owned_lse, grad_query, key_gradient, value_gradient
```

```python
import functools

import jax
import jax.numpy as jnp
from jax import lax
from jax.experimental import pallas as pl
from jax.experimental.pallas import tpu as pltpu
from jax.sharding import PartitionSpec as P

HEAD_SIZE = 128
MASK = -1e30
LOG2E = 1.4426950408889634
LN2 = 0.6931471805599453
NT = (((1,), (1,)), ((), ()))
NN = (((1,), (0,)), ((), ()))


def dot(a, b, dims):
    return lax.dot_general(a, b, dims, preferred_element_type=jnp.float32)


def pack_kernel(copies, groups, k_ref, v_ref, *outs):
    rows, cols = k_ref.shape
    heads = cols // (groups * HEAD_SIZE)
    for g in range(groups):
        for h in range(heads):
            at = (h * groups + g) * HEAD_SIZE
            for c in range(copies):
                dst = pl.ds((c * heads + h) * rows, rows)
                outs[g][dst, :HEAD_SIZE] = k_ref[:, at : at + HEAD_SIZE]
                outs[g][dst, HEAD_SIZE:] = v_ref[:, at : at + HEAD_SIZE]


def pack(key_rows, value_rows, copies, groups, heads):
    rows = key_rows.shape[0]
    return pl.pallas_call(
        functools.partial(pack_kernel, copies, groups),
        out_shape=[
            jax.ShapeDtypeStruct((copies * heads * rows, 2 * HEAD_SIZE), jnp.bfloat16)
        ]
        * groups,
        name="pack",
    )(key_rows, value_rows)


def attention_kernel(
    window, group, shard_ref, start_ref, q_ref, do_ref, kv_ref, *refs
):
    o_ref, lse_ref, dq_ref, dkv_ref, qs, dos, p_all, ds_all, kt, vt = refs[-10:]
    tok = q_ref.shape[0]
    keys = window * tok
    scale = HEAD_SIZE ** (-0.5)
    shard = shard_ref[0]
    first = jnp.maximum(shard - (window - 1), 0) * tok
    first = pl.multiple_of(first, tok)
    for h in range(group):
        cols = slice(h * HEAD_SIZE, (h + 1) * HEAD_SIZE)
        qs[h * tok : (h + 1) * tok, :] = q_ref[:, cols]
        dos[h * tok : (h + 1) * tok, :] = do_ref[:, cols]
    kt[...] = kv_ref[pl.ds(first, keys), :HEAD_SIZE].T
    vt[...] = kv_ref[pl.ds(first, keys), HEAD_SIZE:].T
    pair = 2
    width = pair * tok
    place = first + lax.broadcasted_iota(jnp.int32, (keys, width), 0)
    query = shard * tok + (lax.broadcasted_iota(jnp.int32, (keys, width), 1) & (tok - 1))
    begin = jnp.concatenate([start_ref[...]] * pair, axis=1)
    allowed = (place >= begin) & (place <= query)
    for i in range(group // pair):
        rows = slice(i * width, (i + 1) * width)
        s = dot(kv_ref[pl.ds(first, keys), :HEAD_SIZE], qs[rows, :], NT)
        s = jnp.where(allowed, s * (scale * LOG2E), MASK)
        top = jnp.max(s, axis=0, keepdims=True)
        p = jnp.exp2(s - top)
        total = jnp.sum(p, axis=0, keepdims=True)
        inv = 1.0 / total
        ot = dot(vt[...], p.astype(jnp.bfloat16), NN) * inv
        dp = dot(kv_ref[pl.ds(first, keys), HEAD_SIZE:], dos[rows, :], NT)
        lse = (top + jnp.log2(total)) * LN2
        p = p * inv
        delta = jnp.sum(p * dp, axis=0, keepdims=True)
        ds = (p * (dp - delta)).astype(jnp.bfloat16)
        p_all[:, rows] = p.astype(jnp.bfloat16)
        ds_all[:, rows] = ds
        dqt = dot(kt[...], ds, NN) * scale
        for j in range(pair):
            h = i * pair + j
            cols = slice(h * HEAD_SIZE, (h + 1) * HEAD_SIZE)
            part = slice(j * tok, (j + 1) * tok)
            o_ref[:, cols] = ot[:, part].T.astype(jnp.bfloat16)
            dq_ref[:, cols] = dqt[:, part].T.astype(jnp.bfloat16)
            lse_ref[h : h + 1, :] = lse[:, part]
    dkv_ref[...] = jnp.zeros_like(dkv_ref)
    dkv_ref[pl.ds(first, keys), HEAD_SIZE:] = dot(p_all[...], dos[...], NN).astype(jnp.bfloat16)
    dkv_ref[pl.ds(first, keys), :HEAD_SIZE] = (dot(ds_all[...], qs[...], NN) * scale).astype(
        jnp.bfloat16
    )


def attend(g, group, window, shard, start, queries, grads, kv, held):
    tok = queries.shape[0]
    wide = group * HEAD_SIZE
    keys = window * tok
    column = pl.BlockSpec((tok, wide), lambda i: (0, g))
    whole = lambda shape: pl.BlockSpec(shape, lambda i: (0,) * len(shape))
    anywhere = pl.BlockSpec(memory_space=pl.ANY)
    flops = 12 * group * tok * keys * HEAD_SIZE
    return pl.pallas_call(
        functools.partial(attention_kernel, window, group),
        grid=(1,),
        out_shape=[
            jax.ShapeDtypeStruct(queries.shape, jnp.bfloat16),
            jax.ShapeDtypeStruct((group, tok), jnp.float32),
            jax.ShapeDtypeStruct(queries.shape, jnp.bfloat16),
            jax.ShapeDtypeStruct(kv.shape, jnp.bfloat16),
        ],
        in_specs=[
            pl.BlockSpec(memory_space=pltpu.SMEM),
            whole((1, tok)),
            column,
            column,
            whole(kv.shape),
        ]
        + [anywhere] * len(held),
        out_specs=[column, whole((group, tok)), column, whole(kv.shape)],
        scratch_shapes=[
            pltpu.VMEM((group * tok, HEAD_SIZE), jnp.bfloat16),
            pltpu.VMEM((group * tok, HEAD_SIZE), jnp.bfloat16),
            pltpu.VMEM((keys, group * tok), jnp.bfloat16),
            pltpu.VMEM((keys, group * tok), jnp.bfloat16),
            pltpu.VMEM((HEAD_SIZE, keys), jnp.bfloat16),
            pltpu.VMEM((HEAD_SIZE, keys), jnp.bfloat16),
        ],
        input_output_aliases={5: 0, 6: 2} if held else {},
        cost_estimate=pl.CostEstimate(
            flops=flops, bytes_accessed=4 * tok * wide * 2, transcendentals=group * tok * keys
        ),
        name="attend",
    )(shard, start, queries, grads, kv, *held)


def total_kernel(groups, sources, *refs):
    parts, (dk_ref, dv_ref) = refs[:groups], refs[groups:]
    rows, cols = dk_ref.shape
    heads = cols // (groups * HEAD_SIZE)
    for g in range(groups):
        for h in range(heads):
            total = jnp.zeros((rows, 2 * HEAD_SIZE), jnp.float32)
            for c in range(sources):
                at = (c * heads + h) * rows
                total = total + parts[g][at : at + rows, :].astype(jnp.float32)
            to = (h * groups + g) * HEAD_SIZE
            dk_ref[:, to : to + HEAD_SIZE] = total[:, :HEAD_SIZE].astype(jnp.bfloat16)
            dv_ref[:, to : to + HEAD_SIZE] = total[:, HEAD_SIZE:].astype(jnp.bfloat16)


def body(queries, key_rows, value_rows, grad_out, doc_ids, block_owner):
    shards = lax.axis_size("ctx")
    heads = lax.axis_size("head")
    shard = lax.axis_index("ctx")
    tok = queries.shape[0]
    block = tok // shards
    groups = key_rows.shape[1] // HEAD_SIZE // heads
    group = queries.shape[1] // HEAD_SIZE // groups
    window = shards // 2 + 1
    packed = pack(key_rows, value_rows, shards, groups, heads)
    moved = [
        lax.all_to_all(x.reshape(shards * heads, -1, 2 * HEAD_SIZE), ("ctx", "head"), 0, 0, tiled=True)
        for x in packed
    ]
    mine = lax.dynamic_slice_in_dim(doc_ids, shard * tok, tok)
    start = jnp.sum((doc_ids[:, None] < mine[None, :]).astype(jnp.int32), axis=0, keepdims=True)
    index = shard.reshape(1)
    held, lse, sent = (), [], []
    for g in range(groups):
        kv = moved[g].reshape(-1, 2 * HEAD_SIZE)
        o, norm, dq, dkv = attend(g, group, window, index, start, queries, grad_out, kv, held)
        held = (o, dq)
        lse.append(norm)
        sent.append(
            lax.all_to_all(dkv.reshape(shards * heads, -1, 2 * HEAD_SIZE), ("ctx", "head"), 0, 0, tiled=True)
        )
    natural = jnp.concatenate(lse, axis=0).reshape(groups * group, shards, block)
    owner = lax.dynamic_index_in_dim(block_owner, shard, 0, keepdims=False)
    pick = owner[None, :] == jnp.arange(shards, dtype=jnp.int32)[:, None]
    chosen = jnp.sum(
        jnp.where(pick[:, None, :, None], natural[None], 0.0), axis=2
    )
    owned = lax.all_to_all(chosen.reshape(shards, 1, -1), "ctx", 0, 0, tiled=True)
    owned = owned.reshape(shards, groups * group, block).transpose(1, 0, 2).reshape(-1, tok)
    dk, dv = pl.pallas_call(
        functools.partial(total_kernel, groups, shards),
        out_shape=[jax.ShapeDtypeStruct(key_rows.shape, jnp.bfloat16)] * 2,
        name="total",
    )(*[x.reshape(-1, 2 * HEAD_SIZE) for x in sent])
    return (held[0], owned, held[1], dk, dv)


def solution(mesh):
    return jax.shard_map(
        body,
        mesh=mesh,
        in_specs=(
            P("ctx", "head"),
            P(("ctx", "head"), None),
            P(("ctx", "head"), None),
            P("ctx", "head"),
            P(),
            P(),
        ),
        out_specs=(
            P("ctx", "head"),
            P("head", "ctx"),
            P("ctx", "head"),
            P(("ctx", "head"), None),
            P(("ctx", "head"), None),
        ),
        check_vma=False,
    )
```

```python
import functools

import jax
import jax.numpy as jnp
from jax import lax
from jax.experimental import pallas as pl
from jax.experimental.pallas import tpu as pltpu
from jax.sharding import Mesh
from jax.sharding import PartitionSpec as P

HEAD_SIZE = 128
MASK = -1e30
LOG2E = 1.4426950408889634
LN2 = 0.6931471805599453
NT = (((1,), (1,)), ((), ()))
NN = (((1,), (0,)), ((), ()))
CTX = ("half", "sub")


def dot(a, b, dims):
    return lax.dot_general(a, b, dims, preferred_element_type=jnp.float32)


def room(extra):
    return pltpu.CompilerParams(vmem_limit_bytes=min((6 << 20) + extra, 60 << 20))


def pack_kernel(groups, k_hbm, v_hbm, out_ref, k_ref, v_ref, sems):
    copies, heads = out_ref.shape[:2]
    loads = [
        pltpu.make_async_copy(k_hbm, k_ref, sems.at[0]),
        pltpu.make_async_copy(v_hbm, v_ref, sems.at[1]),
    ]
    for load in loads:
        load.start()
    for load in loads:
        load.wait()
    for g in range(groups):
        for h in range(heads):
            at = (h * groups + g) * HEAD_SIZE
            to = 2 * g * HEAD_SIZE
            for c in range(copies):
                out_ref[c, h, :, to : to + HEAD_SIZE] = k_ref[:, at : at + HEAD_SIZE]
                out_ref[c, h, :, to + HEAD_SIZE : to + 2 * HEAD_SIZE] = v_ref[
                    :, at : at + HEAD_SIZE
                ]


def attention_kernel(group, far, half_ref, base_ref, start_ref, q_ref, do_ref, near_ref, *refs):
    far_refs, refs = refs[:far], refs[far:]
    o_ref, lse_ref, dq_ref, dnear_ref = refs[:4]
    dfar_refs, refs = refs[4 : 4 + far], refs[4 + far :]
    qs, dos, kw, vw, kt, vt, bias, p_all, ds_all = refs
    tok = q_ref.shape[0]
    keys = kw.shape[0]
    scale = HEAD_SIZE ** (-0.5)
    half = half_ref[0]
    for h in range(group):
        cols = slice(h * HEAD_SIZE, (h + 1) * HEAD_SIZE)
        qs[h * tok : (h + 1) * tok, :] = q_ref[:, cols]
        dos[h * tok : (h + 1) * tok, :] = do_ref[:, cols]
    blocks = [near_ref.at[half], near_ref.at[1 - half], *far_refs]
    for b, ref in enumerate(blocks):
        rows = slice(b * tok, (b + 1) * tok)
        kw[rows, :] = ref[:, :HEAD_SIZE]
        vw[rows, :] = ref[:, HEAD_SIZE:]
    kt[...] = kw[...].T
    vt[...] = vw[...].T

    @pl.when(pl.program_id(0) == 0)
    def _():
        row = lax.broadcasted_iota(jnp.int32, (tok, tok), 0)
        query = base_ref[0] + lax.broadcasted_iota(jnp.int32, (tok, tok), 1)
        for b in range(len(blocks)):
            place = base_ref[b] + row
            allowed = (place >= start_ref[...]) & (place <= query)
            bias[b * tok : (b + 1) * tok, :] = jnp.where(allowed, 0.0, MASK)

    pair = 2
    width = pair * tok
    count = group // pair

    def at(i):
        return slice(i * width, (i + 1) * width)

    def scores(i):
        return dot(kw[...], qs[at(i), :], NT)

    def finish(i, p, inv, dp):
        low = p_all[:, at(i)]
        ot = dot(vt[...], low, NN)
        outs = [ot[:, j * tok : (j + 1) * tok].T.astype(jnp.bfloat16) for j in range(pair)]
        turned = ot.astype(jnp.bfloat16).astype(jnp.float32)
        grad = dos[at(i), :].T.astype(jnp.float32)
        delta = jnp.sum(turned * grad, axis=0, keepdims=True)
        ds_all[:, at(i)] = ((p * inv) * (dp - delta)).astype(jnp.bfloat16)
        dqt = dot(kt[...], ds_all[:, at(i)], NN) * scale
        for j in range(pair):
            h = i * pair + j
            cols = slice(h * HEAD_SIZE, (h + 1) * HEAD_SIZE)
            o_ref[:, cols] = outs[j]
            dq_ref[:, cols] = dqt[:, j * tok : (j + 1) * tok].T.astype(jnp.bfloat16)

    following = scores(0)
    waiting = []
    for i in range(count):
        s = following
        if i + 1 < count:
            following = scores(i + 1)
        dp = dot(vw[...], dos[at(i), :], NT)
        s = s * (scale * LOG2E) + jnp.concatenate([bias[...]] * pair, axis=1)
        top = jnp.max(s, axis=0, keepdims=True)
        p = jnp.exp2(s - top)
        total = jnp.sum(p, axis=0, keepdims=True)
        inv = 1.0 / total
        lse = (top + jnp.log2(total)) * LN2
        for j in range(pair):
            lse_ref[i * pair + j : i * pair + j + 1, :] = lse[:, j * tok : (j + 1) * tok]
        p_all[:, at(i)] = (p * inv).astype(jnp.bfloat16)

        waiting.append((i, p, inv, dp))
        if i + 1 == count:
            dv = dot(p_all[...], dos[...], NN).astype(jnp.bfloat16)
        if len(waiting) > 0:
            finish(*waiting.pop(0))
    while waiting:
        finish(*waiting.pop(0))
    dk = (dot(ds_all[...], qs[...], NN) * scale).astype(jnp.bfloat16)
    for b, ref in enumerate([dnear_ref.at[0], dnear_ref.at[1], *dfar_refs]):
        rows = slice(b * tok, (b + 1) * tok)
        ref[:, :HEAD_SIZE] = dk[rows]
        ref[:, HEAD_SIZE:] = dv[rows]


def attend(groups, half, base, start, queries, grads, near, far):
    tok = queries.shape[0]
    group = queries.shape[1] // HEAD_SIZE // groups
    keys = (2 + len(far)) * tok
    column = pl.BlockSpec((tok, group * HEAD_SIZE), lambda g: (0, g))
    pair = pl.BlockSpec((2, tok, 2 * HEAD_SIZE), lambda g: (0, 0, g))
    single = pl.BlockSpec((tok, 2 * HEAD_SIZE), lambda g: (0, g))
    scalar = pl.BlockSpec(memory_space=pltpu.SMEM)
    wide = jax.ShapeDtypeStruct(queries.shape, jnp.bfloat16)
    rows = group * tok
    bf = lambda *shape: pltpu.VMEM(shape, jnp.bfloat16)
    return pl.pallas_call(
        functools.partial(attention_kernel, group, len(far)),
        grid=(groups,),
        out_shape=[
            wide,
            jax.ShapeDtypeStruct((groups * group, tok), jnp.float32),
            wide,
            jax.ShapeDtypeStruct(near.shape, jnp.bfloat16),
        ]
        + [jax.ShapeDtypeStruct(x.shape, jnp.bfloat16) for x in far],
        in_specs=[
            scalar,
            scalar,
            pl.BlockSpec((1, tok), lambda g: (0, 0)),
            column,
            column,
            pair,
        ]
        + [single] * len(far),
        out_specs=[column, pl.BlockSpec((group, tok), lambda g: (g, 0)), column, pair]
        + [single] * len(far),
        scratch_shapes=[
            bf(rows, HEAD_SIZE),
            bf(rows, HEAD_SIZE),
            bf(keys, HEAD_SIZE),
            bf(keys, HEAD_SIZE),
            bf(HEAD_SIZE, keys),
            bf(HEAD_SIZE, keys),
            pltpu.VMEM((keys, tok), jnp.float32),
            bf(keys, rows),
            bf(keys, rows),
        ],
        cost_estimate=pl.CostEstimate(
            flops=12 * groups * rows * keys * HEAD_SIZE,
            bytes_accessed=16 * groups * rows * HEAD_SIZE,
            transcendentals=groups * rows * keys,
        ),
        compiler_params=room(16 * keys * rows),
        name="attend",
    )(half, base, start, queries, grads, near, *far)


def collect_kernel(near_ref, flag_ref, half_ref, *refs):
    out_ref, refs = refs[-1], refs[:-1]
    half = half_ref[0]
    own = near_ref[0].astype(jnp.float32)
    low = near_ref[1].astype(jnp.float32)
    for d, ref in enumerate(refs):
        got = ref[...].astype(jnp.float32)
        first = flag_ref[d] == 1
        own = own + jnp.where(first, got, 0.0)
        low = low + jnp.where(first, 0.0, got)
    out_ref[half] = own.astype(jnp.bfloat16)
    out_ref[1 - half] = low.astype(jnp.bfloat16)


def finish_kernel(groups, part_ref, dk_ref, dv_ref):
    for h in range(part_ref.shape[1]):
        total = part_ref[0, h].astype(jnp.float32) + part_ref[1, h].astype(jnp.float32)
        total = total.astype(jnp.bfloat16)
        for g in range(groups):
            to = (h * groups + g) * HEAD_SIZE
            at = 2 * g * HEAD_SIZE
            dk_ref[:, to : to + HEAD_SIZE] = total[:, at : at + HEAD_SIZE]
            dv_ref[:, to : to + HEAD_SIZE] = total[:, at + HEAD_SIZE : at + 2 * HEAD_SIZE]


def body(queries, key_rows, value_rows, grad_out, doc_ids, block_owner):
    subs = lax.axis_size("sub")
    shards = 2 * subs
    heads = lax.axis_size("head")
    half = lax.axis_index("half")
    sub = lax.axis_index("sub")
    shard = half * subs + sub
    tok = queries.shape[0]
    rows = key_rows.shape[0]
    block = tok // shards
    groups = key_rows.shape[1] // HEAD_SIZE // heads
    width = 2 * groups * HEAD_SIZE
    packed = pl.pallas_call(
        functools.partial(pack_kernel, groups),
        out_shape=jax.ShapeDtypeStruct((2, heads, rows, width), jnp.bfloat16),
        in_specs=[pl.BlockSpec(memory_space=pltpu.HBM)] * 2,
        scratch_shapes=[pltpu.VMEM(key_rows.shape, jnp.bfloat16)] * 2
        + [pltpu.SemaphoreType.DMA((2,))],
        compiler_params=room(8 * rows * heads * width),
        name="pack",
    )(key_rows, value_rows)
    near = lax.all_to_all(
        packed.reshape(2 * heads, rows, width), ("half", "head"), 0, 0, tiled=True
    ).reshape(2, tok, width)

    def swap(x, d):
        return lax.ppermute(x, "sub", [(i, i ^ d) for i in range(subs)])

    steps = range(1, subs)
    earlier = [sub < (sub ^ d) for d in steps]
    chosen = {}
    far = []
    for d in steps:
        bit = d.bit_length() - 1
        if bit not in chosen:
            chosen[bit] = lax.dynamic_index_in_dim(
                near, jnp.where(earlier[d - 1], half, 1 - half), 0, keepdims=False
            )
        far.append(swap(chosen[bit], d))
    mine = lax.dynamic_slice_in_dim(doc_ids, shard * tok, tok)
    start = jnp.sum((doc_ids[:, None] < mine[None, :]).astype(jnp.int32), axis=0, keepdims=True)
    bases = [shard, shard - subs]
    for d in steps:
        partner = half * subs + (sub ^ d)
        bases.append(jnp.where(earlier[d - 1], partner - subs, partner))
    base = jnp.stack(bases) * tok
    half_index = half.reshape(1)
    flags = jnp.stack(earlier).astype(jnp.int32)
    attention, norm, dq, dnear, *dfar = attend(
        groups, half_index, base, start, queries, grad_out, near, far
    )
    returned = [swap(x, d) for d, x in zip(steps, dfar, strict=True)]
    natural = norm.reshape(norm.shape[0], shards, block)
    owner = lax.dynamic_index_in_dim(block_owner, shard, 0, keepdims=False)
    order = jnp.stack([(sub ^ d) + subs * e for d in range(subs) for e in range(2)])
    pick = owner[None, :] == order[:, None]
    routed = jnp.sum(jnp.where(pick[:, None, :, None], natural[None], 0.0), axis=2)
    routed = routed.reshape(subs, 2, -1)
    near_lse = jnp.stack([routed[0]] + [swap(routed[d], d) for d in steps])
    across = lax.dynamic_index_in_dim(near_lse, 1 - half, 1, keepdims=False)
    across = lax.ppermute(across, "half", [(0, 1), (1, 0)])
    kept = lax.dynamic_index_in_dim(near_lse, half, 1, keepdims=False)
    both = jnp.concatenate([kept, across], axis=0)
    source = jnp.stack([(sub ^ d) + subs * e for e in (half, 1 - half) for d in range(subs)])
    place = source[None, :] == jnp.arange(shards, dtype=jnp.int32)[:, None]
    owned = jnp.sum(jnp.where(place[:, :, None], both[None], 0.0), axis=1)
    owned = owned.reshape(shards, -1, block).transpose(1, 0, 2).reshape(-1, tok)
    vmem = pl.BlockSpec(memory_space=pltpu.VMEM)
    scalar = pl.BlockSpec(memory_space=pltpu.SMEM)
    summed = pl.pallas_call(
        collect_kernel,
        out_shape=jax.ShapeDtypeStruct(near.shape, jnp.bfloat16),
        in_specs=[vmem, scalar, scalar] + [vmem] * len(returned),
        out_specs=vmem,
        compiler_params=room(8 * near.size),
        name="collect",
    )(dnear, flags, half_index, *returned)
    parts = lax.all_to_all(
        summed.reshape(2 * heads, rows, width), ("half", "head"), 0, 0, tiled=True
    )
    dk, dv = pl.pallas_call(
        functools.partial(finish_kernel, groups),
        out_shape=[jax.ShapeDtypeStruct(key_rows.shape, jnp.bfloat16)] * 2,
        compiler_params=room(8 * near.size),
        name="finish",
    )(parts.reshape(2, heads, rows, width))
    return (attention, owned, dq, dk, dv)


def solution(mesh):
    shards, heads = mesh.shape["ctx"], mesh.shape["head"]
    inner = Mesh(mesh.devices.reshape(2, shards // 2, heads), (*CTX, "head"))
    rows = P((*CTX, "head"), None)
    return jax.shard_map(
        body,
        mesh=inner,
        in_specs=(P(CTX, "head"), rows, rows, P(CTX, "head"), P(), P()),
        out_specs=(P(CTX, "head"), P("head", CTX), P(CTX, "head"), rows, rows),
        check_vma=False,
    )
```

```python
import functools

import jax
import jax.numpy as jnp
from jax import lax
from jax.experimental import pallas as pl
from jax.experimental.pallas import tpu as pltpu
from jax.sharding import Mesh
from jax.sharding import PartitionSpec as P

HEAD_SIZE = 128
MASK = -1e30
LOG2E = 1.4426950408889634
LN2 = 0.6931471805599453
NT = (((1,), (1,)), ((), ()))
NN = (((1,), (0,)), ((), ()))
CTX = ("half", "sub")


def dot(a, b, dims):
    return lax.dot_general(a, b, dims, preferred_element_type=jnp.float32)


def room(extra):
    return pltpu.CompilerParams(vmem_limit_bytes=min((6 << 20) + extra, 60 << 20))


def own_kernel(groups, where_ref, k_ref, v_ref, mine_ref, *own_refs):
    heads = mine_ref.shape[0]
    for g in range(groups):
        for part, ref in enumerate((k_ref, v_ref)):
            to = slice((2 * g + part) * HEAD_SIZE, (2 * g + part + 1) * HEAD_SIZE)
            for h in range(heads):
                at = (h * groups + g) * HEAD_SIZE
                mine_ref[h, :, to] = ref[:, at : at + HEAD_SIZE]
            for o, own in enumerate(own_refs):
                at = pl.multiple_of(((where_ref[2] ^ o) * groups + g) * HEAD_SIZE, HEAD_SIZE)
                own[:, to] = ref[:, pl.ds(at, HEAD_SIZE)]


def far_kernel(groups, where_ref, mine_ref, kl_ref, vl_ref, far_ref):
    subs, heads = far_ref.shape[:2]
    for g in range(groups):
        for part, low in enumerate((kl_ref, vl_ref)):
            to = slice((2 * g + part) * HEAD_SIZE, (2 * g + part + 1) * HEAD_SIZE)
            for h in range(heads):
                at = (h * groups + g) * HEAD_SIZE
                mine = mine_ref[h, :, to]
                theirs = low[:, at : at + HEAD_SIZE]
                for dest in range(subs):
                    far_ref[dest, h, :, to] = jnp.where(where_ref[1] < dest, mine, theirs)


def attention_kernel(group, heads, where_ref, base_ref, start_ref, q_ref, do_ref, far_ref, *refs):
    own_refs, refs = refs[:heads], refs[heads:]
    o_ref, lse_ref, dq_ref, dfar_ref = refs[:4]
    down_refs, refs = refs[4 : 4 + heads], refs[4 + heads :]
    qs, dos, kw, vw, kt, vt, bias, p_all, ds_all = refs
    tok = q_ref.shape[0]
    scale = HEAD_SIZE ** (-0.5)
    subs = far_ref.shape[0]
    piece = tok // heads
    for h in range(group):
        cols = slice(h * HEAD_SIZE, (h + 1) * HEAD_SIZE)
        qs[h * tok : (h + 1) * tok, :] = q_ref[:, cols]
        dos[h * tok : (h + 1) * tok, :] = do_ref[:, cols]
    for b in range(subs):
        rows = slice(b * tok, (b + 1) * tok)
        kw[rows, :] = far_ref[b, :, :HEAD_SIZE]
        vw[rows, :] = far_ref[b, :, HEAD_SIZE:]

    def held(o):
        return pl.ds(pl.multiple_of(subs * tok + (where_ref[2] ^ o) * piece, piece), piece)

    for o, ref in enumerate(own_refs):
        kw[held(o), :] = ref[:, :HEAD_SIZE]
        vw[held(o), :] = ref[:, HEAD_SIZE:]
    kt[...] = kw[...].T
    vt[...] = vw[...].T

    @pl.when(pl.program_id(0) == 0)
    def _():
        row = lax.broadcasted_iota(jnp.int32, (tok, tok), 0)
        query = base_ref[subs] + lax.broadcasted_iota(jnp.int32, (tok, tok), 1)
        for b in range(subs + 1):
            place = base_ref[b] + row
            allowed = (place >= start_ref[...]) & (place <= query)
            bias[b * tok : (b + 1) * tok, :] = jnp.where(allowed, 0.0, MASK)

    pair = 2
    width = pair * tok
    count = group // pair

    def at(i):
        return slice(i * width, (i + 1) * width)

    def scores(i):
        return dot(kw[...], qs[at(i), :], NT)

    def finish(i, p, inv, dp):
        low = p_all[:, at(i)]
        ot = dot(vt[...], low, NN)
        outs = [ot[:, j * tok : (j + 1) * tok].T.astype(jnp.bfloat16) for j in range(pair)]
        turned = ot.astype(jnp.bfloat16).astype(jnp.float32)
        grad = dos[at(i), :].T.astype(jnp.float32)
        delta = jnp.sum(turned * grad, axis=0, keepdims=True)
        ds_all[:, at(i)] = ((p * inv) * (dp - delta)).astype(jnp.bfloat16)
        dqt = dot(kt[...], ds_all[:, at(i)], NN) * scale
        for j in range(pair):
            h = i * pair + j
            cols = slice(h * HEAD_SIZE, (h + 1) * HEAD_SIZE)
            o_ref[:, cols] = outs[j]
            dq_ref[:, cols] = dqt[:, j * tok : (j + 1) * tok].T.astype(jnp.bfloat16)

    following = scores(0)
    waiting = []
    for i in range(count):
        s = following
        if i + 1 < count:
            following = scores(i + 1)
        dp = dot(vw[...], dos[at(i), :], NT)
        s = s * (scale * LOG2E) + jnp.concatenate([bias[...]] * pair, axis=1)
        top = jnp.max(s, axis=0, keepdims=True)
        p = jnp.exp2(s - top)
        total = jnp.sum(p, axis=0, keepdims=True)
        inv = 1.0 / total
        lse = (top + jnp.log2(total)) * LN2
        for j in range(pair):
            lse_ref[i * pair + j : i * pair + j + 1, :] = lse[:, j * tok : (j + 1) * tok]
        p_all[:, at(i)] = (p * inv).astype(jnp.bfloat16)

        waiting.append((i, p, inv, dp))
        if i + 1 == count:
            dv = dot(p_all[...], dos[...], NN).astype(jnp.bfloat16)
        if len(waiting) > 0:
            finish(*waiting.pop(0))
    while waiting:
        finish(*waiting.pop(0))
    kw[...] = (dot(ds_all[...], qs[...], NN) * scale).astype(jnp.bfloat16)
    vw[...] = dv
    for b in range(subs):
        rows = slice(b * tok, (b + 1) * tok)
        dfar_ref[b, :, :HEAD_SIZE] = kw[rows, :]
        dfar_ref[b, :, HEAD_SIZE:] = vw[rows, :]
    for o, ref in enumerate(down_refs):
        ref[:, :HEAD_SIZE] = kw[held(o), :]
        ref[:, HEAD_SIZE:] = vw[held(o), :]


def attend(groups, where, base, start, queries, grads, far, own):
    tok = queries.shape[0]
    group = queries.shape[1] // HEAD_SIZE // groups
    keys = (1 + far.shape[0]) * tok
    column = pl.BlockSpec((tok, group * HEAD_SIZE), lambda g: (0, g))
    many = pl.BlockSpec((far.shape[0], tok, 2 * HEAD_SIZE), lambda g: (0, 0, g))
    single = pl.BlockSpec((own[0].shape[0], 2 * HEAD_SIZE), lambda g: (0, g))
    scalar = pl.BlockSpec(memory_space=pltpu.SMEM)
    wide = jax.ShapeDtypeStruct(queries.shape, jnp.bfloat16)
    rows = group * tok
    bf = lambda *shape: pltpu.VMEM(shape, jnp.bfloat16)
    return pl.pallas_call(
        functools.partial(attention_kernel, group, len(own)),
        grid=(groups,),
        out_shape=[
            wide,
            jax.ShapeDtypeStruct((groups * group, tok), jnp.float32),
            wide,
            jax.ShapeDtypeStruct(far.shape, jnp.bfloat16),
        ]
        + [jax.ShapeDtypeStruct(x.shape, jnp.bfloat16) for x in own],
        in_specs=[
            scalar,
            scalar,
            pl.BlockSpec((1, tok), lambda g: (0, 0)),
            column,
            column,
            many,
        ]
        + [single] * len(own),
        out_specs=[column, pl.BlockSpec((group, tok), lambda g: (g, 0)), column, many]
        + [single] * len(own),
        scratch_shapes=[
            bf(rows, HEAD_SIZE),
            bf(rows, HEAD_SIZE),
            bf(keys, HEAD_SIZE),
            bf(keys, HEAD_SIZE),
            bf(HEAD_SIZE, keys),
            bf(HEAD_SIZE, keys),
            pltpu.VMEM((keys, tok), jnp.float32),
            bf(keys, rows),
            bf(keys, rows),
        ],
        cost_estimate=pl.CostEstimate(
            flops=12 * groups * rows * keys * HEAD_SIZE,
            bytes_accessed=16 * groups * rows * HEAD_SIZE,
            transcendentals=groups * rows * keys,
        ),
        compiler_params=room(16 * keys * rows),
        name="attend",
    )(where, base, start, queries, grads, far, *own)


def collect_kernel(groups, where_ref, far_ref, *refs):
    heads = far_ref.shape[1]
    own_refs, (low_ref, sum_ref) = refs[:heads], refs[heads:]
    sub, head = where_ref[1], where_ref[2]
    pieces = [(g, part) for g in range(groups) for part in range(2)]
    for o, ref in enumerate(own_refs):
        for g, part in pieces:
            at = pl.multiple_of(((head ^ o) * groups + g) * HEAD_SIZE, HEAD_SIZE)
            to = (2 * g + part) * HEAD_SIZE
            sum_ref[part, :, pl.ds(at, HEAD_SIZE)] = ref[
                :, to : to + HEAD_SIZE
            ].astype(jnp.float32)
    for h in range(heads):
        for g, part in pieces:
            at = (h * groups + g) * HEAD_SIZE
            cols = slice(at, at + HEAD_SIZE)
            to = (2 * g + part) * HEAD_SIZE
            own = sum_ref[part, :, cols]
            low = jnp.zeros_like(own)
            for s in range(far_ref.shape[0]):
                got = far_ref[s, h, :, to : to + HEAD_SIZE].astype(jnp.float32)
                own = own + jnp.where(sub < s, got, 0.0)
                low = low + jnp.where(sub < s, 0.0, got)
            sum_ref[part, :, cols] = own
            low_ref[part, :, cols] = low.astype(jnp.bfloat16)


def finish_kernel(low_ref, sum_ref, dk_ref, dv_ref):
    for part, ref in enumerate((dk_ref, dv_ref)):
        ref[...] = (sum_ref[part] + low_ref[part].astype(jnp.float32)).astype(jnp.bfloat16)


def body(queries, key_rows, value_rows, grad_out, doc_ids, block_owner):
    subs = lax.axis_size("sub")
    shards = 2 * subs
    heads = lax.axis_size("head")
    half, sub, head = (lax.axis_index(name) for name in (*CTX, "head"))
    shard = half * subs + sub
    tok = queries.shape[0]
    rows = key_rows.shape[0]
    block = tok // shards
    groups = key_rows.shape[1] // HEAD_SIZE // heads
    width = 2 * groups * HEAD_SIZE
    where = jnp.stack([half, sub, head])
    vmem = pl.BlockSpec(memory_space=pltpu.VMEM)
    scalar = pl.BlockSpec(memory_space=pltpu.SMEM)

    def swap(x, axis, d):
        return lax.ppermute(x, axis, [(i, i ^ d) for i in range(lax.axis_size(axis))])

    low_keys, low_values = swap(key_rows, "half", 1), swap(value_rows, "half", 1)
    mine, *own = pl.pallas_call(
        functools.partial(own_kernel, groups),
        out_shape=[jax.ShapeDtypeStruct((heads, rows, width), jnp.bfloat16)]
        + [jax.ShapeDtypeStruct((rows, width), jnp.bfloat16)] * heads,
        in_specs=[scalar] + [vmem] * 2,
        cost_estimate=pl.CostEstimate(
            flops=1 << 21, bytes_accessed=12 * key_rows.size, transcendentals=0
        ),
        compiler_params=room(16 * key_rows.size),
        name="own",
    )(where, key_rows, value_rows)
    own = [own[0]] + [swap(own[o], "head", o) for o in range(1, heads)]
    packed = pl.pallas_call(
        functools.partial(far_kernel, groups),
        out_shape=jax.ShapeDtypeStruct((subs, heads, rows, width), jnp.bfloat16),
        in_specs=[scalar] + [vmem] * 3,
        compiler_params=room(8 * subs * rows * heads * width),
        name="far",
    )(where, mine, low_keys, low_values)
    far = lax.all_to_all(
        packed.reshape(subs * heads, rows, width), ("sub", "head"), 0, 0, tiled=True
    ).reshape(subs, tok, width)
    mine = lax.dynamic_slice_in_dim(doc_ids, shard * tok, tok)
    start = jnp.sum((doc_ids[:, None] < mine[None, :]).astype(jnp.int32), axis=0, keepdims=True)
    each = jnp.arange(subs + 1, dtype=jnp.int32)
    base = half * subs + jnp.where(each < subs, each - jnp.where(each >= sub, subs, 0), sub)
    attention, norm, dq, dfar, *down = attend(
        groups, where, base * tok, start, queries, grad_out, far, own
    )
    parts = lax.all_to_all(
        dfar.reshape(subs * heads, rows, width), ("sub", "head"), 0, 0, tiled=True
    )
    down = [down[0]] + [swap(down[o], "head", o) for o in range(1, heads)]
    natural = norm.reshape(norm.shape[0], shards, block)
    owner = lax.dynamic_index_in_dim(block_owner, shard, 0, keepdims=False)
    order = jnp.stack([(sub ^ d) + subs * e for e in (half, 1 - half) for d in range(subs)])
    pick = owner[None, :] == order[:, None]
    routed = jnp.sum(jnp.where(pick[:, None, :, None], natural[None], 0.0), axis=2)
    routed = routed.reshape(2, subs, -1)
    across = swap(routed[1], "half", 1)
    ready = jnp.stack([routed[0], across], axis=1)
    near_lse = [ready[0]] + [swap(ready[d], "sub", d) for d in range(1, subs)]
    both = jnp.concatenate(near_lse, axis=0)
    source = jnp.stack([(sub ^ d) + subs * e for d in range(subs) for e in (half, 1 - half)])
    place = source[None, :] == jnp.arange(shards, dtype=jnp.int32)[:, None]
    owned = jnp.sum(jnp.where(place[:, :, None], both[None], 0.0), axis=1)
    owned = owned.reshape(shards, -1, block).transpose(1, 0, 2).reshape(-1, tok)
    low, sums = pl.pallas_call(
        functools.partial(collect_kernel, groups),
        out_shape=[
            jax.ShapeDtypeStruct((2, *key_rows.shape), jnp.bfloat16),
            jax.ShapeDtypeStruct((2, *key_rows.shape), jnp.float32),
        ],
        in_specs=[scalar] + [vmem] * (1 + heads),
        compiler_params=room(8 * far.size),
        name="collect",
    )(where, parts.reshape(subs, heads, rows, width), *down)
    low = swap(low, "half", 1)
    dk, dv = pl.pallas_call(
        finish_kernel,
        out_shape=[jax.ShapeDtypeStruct(key_rows.shape, jnp.bfloat16)] * 2,
        compiler_params=room(32 * key_rows.size),
        name="finish",
    )(low, sums)
    return (attention, owned, dq, dk, dv)


def solution(mesh):
    shards, heads = mesh.shape["ctx"], mesh.shape["head"]
    inner = Mesh(mesh.devices.reshape(2, shards // 2, heads), (*CTX, "head"))
    rows = P((*CTX, "head"), None)

    return jax.shard_map(
        body,
        mesh=inner,
        in_specs=(P(CTX, "head"), rows, rows, P(CTX, "head"), P(), P()),
        out_specs=(P(CTX, "head"), P("head", CTX), P(CTX, "head"), rows, rows),
        check_vma=False,
    )
```

```python
import functools

import jax
import jax.numpy as jnp
from jax import lax
from jax.experimental import pallas as pl
from jax.experimental.pallas import tpu as pltpu
from jax.sharding import Mesh
from jax.sharding import PartitionSpec as P

HEAD_SIZE = 128
MASK = -1e30
LOG2E = 1.4426950408889634
LN2 = 0.6931471805599453
NT = (((1,), (1,)), ((), ()))
NN = (((1,), (0,)), ((), ()))
CTX = ("half", "sub")


def dot(a, b, dims):
    return lax.dot_general(a, b, dims, preferred_element_type=jnp.float32)


def room(extra):
    return pltpu.CompilerParams(vmem_limit_bytes=min((6 << 20) + extra, 60 << 20))


def own_kernel(groups, where_ref, k_ref, v_ref, mine_ref, *own_refs):
    heads = mine_ref.shape[0]
    for g in range(groups):
        for part, ref in enumerate((k_ref, v_ref)):
            to = slice((2 * g + part) * HEAD_SIZE, (2 * g + part + 1) * HEAD_SIZE)
            for h in range(heads):
                at = (h * groups + g) * HEAD_SIZE
                mine_ref[h, :, to] = ref[:, at : at + HEAD_SIZE]
            for o, own in enumerate(own_refs):
                at = pl.multiple_of(((where_ref[2] ^ o) * groups + g) * HEAD_SIZE, HEAD_SIZE)
                own[:, to] = ref[:, pl.ds(at, HEAD_SIZE)]


def far_kernel(groups, where_ref, mine_ref, kl_ref, vl_ref, far_ref):
    subs, heads = far_ref.shape[:2]
    for g in range(groups):
        for part, low in enumerate((kl_ref, vl_ref)):
            to = slice((2 * g + part) * HEAD_SIZE, (2 * g + part + 1) * HEAD_SIZE)
            for h in range(heads):
                at = (h * groups + g) * HEAD_SIZE
                mine = mine_ref[h, :, to]
                theirs = low[:, at : at + HEAD_SIZE]
                for dest in range(subs):
                    far_ref[dest, h, :, to] = jnp.where(where_ref[1] < dest, mine, theirs)


def attention_kernel(group, groups, heads, *refs):
    scratch = refs[-8 * groups :]
    bias, refs = refs[-8 * groups - 1], refs[: -8 * groups - 1]
    for g in range(groups):
        one_group(g, group, heads, bias, scratch[8 * g : 8 * g + 8], *refs)


def one_group(
    g, group, heads, bias, scratch, where_ref, base_ref, start_ref, q_ref, do_ref, far_ref, *refs
):
    own_refs, refs = refs[:heads], refs[heads:]
    o_ref, lse_ref, dq_ref, dfar_ref = refs[:4]
    down_refs = refs[4:]
    qs, dos, kw, vw, kt, vt, p_all, ds_all = scratch
    key_cols = slice(2 * g * HEAD_SIZE, (2 * g + 1) * HEAD_SIZE)
    value_cols = slice((2 * g + 1) * HEAD_SIZE, (2 * g + 2) * HEAD_SIZE)

    def columns(h):
        return slice((g * group + h) * HEAD_SIZE, (g * group + h + 1) * HEAD_SIZE)

    tok = q_ref.shape[0]
    scale = HEAD_SIZE ** (-0.5)
    subs = far_ref.shape[0]
    piece = tok // heads
    for h in range(group):
        qs[h * tok : (h + 1) * tok, :] = q_ref[:, columns(h)]
        dos[h * tok : (h + 1) * tok, :] = do_ref[:, columns(h)]
    for b in range(subs):
        rows = slice(b * tok, (b + 1) * tok)
        kw[rows, :] = far_ref[b, :, key_cols]
        vw[rows, :] = far_ref[b, :, value_cols]

    def held(o):
        return pl.ds(pl.multiple_of(subs * tok + (where_ref[2] ^ o) * piece, piece), piece)

    for o, ref in enumerate(own_refs):
        kw[held(o), :] = ref[:, key_cols]
        vw[held(o), :] = ref[:, value_cols]
    kt[...] = kw[...].T
    vt[...] = vw[...].T

    if g == 0:
        row = lax.broadcasted_iota(jnp.int32, (tok, tok), 0)
        query = base_ref[subs] + lax.broadcasted_iota(jnp.int32, (tok, tok), 1)
        for b in range(subs + 1):
            place = base_ref[b] + row
            allowed = (place >= start_ref[...]) & (place <= query)
            bias[b * tok : (b + 1) * tok, :] = jnp.where(allowed, 0.0, MASK)

    pair = 2
    width = pair * tok
    count = group // pair

    def at(i):
        return slice(i * width, (i + 1) * width)

    def scores(i):
        return dot(kw[...], qs[at(i), :], NT)

    def finish(i, p, inv, dp):
        low = p_all[:, at(i)]
        ot = dot(vt[...], low, NN)
        outs = [ot[:, j * tok : (j + 1) * tok].T.astype(jnp.bfloat16) for j in range(pair)]
        turned = ot.astype(jnp.bfloat16).astype(jnp.float32)
        grad = dos[at(i), :].T.astype(jnp.float32)
        delta = jnp.sum(turned * grad, axis=0, keepdims=True)
        ds_all[:, at(i)] = ((p * inv) * (dp - delta)).astype(jnp.bfloat16)
        dqt = dot(kt[...], ds_all[:, at(i)], NN) * scale
        for j in range(pair):
            h = i * pair + j
            o_ref[:, columns(h)] = outs[j]
            dq_ref[:, columns(h)] = dqt[:, j * tok : (j + 1) * tok].T.astype(jnp.bfloat16)

    following = scores(0)
    waiting = []
    for i in range(count):
        s = following
        if i + 1 < count:
            following = scores(i + 1)
        dp = dot(vw[...], dos[at(i), :], NT)
        s = s * (scale * LOG2E) + jnp.concatenate([bias[...]] * pair, axis=1)
        top = jnp.max(s, axis=0, keepdims=True)
        p = jnp.exp2(s - top)
        total = jnp.sum(p, axis=0, keepdims=True)
        inv = 1.0 / total
        lse = (top + jnp.log2(total)) * LN2
        for j in range(pair):
            h = g * group + i * pair + j
            lse_ref[h : h + 1, :] = lse[:, j * tok : (j + 1) * tok]
        p_all[:, at(i)] = (p * inv).astype(jnp.bfloat16)

        waiting.append((i, p, inv, dp))
        if i + 1 == count:
            dv = dot(p_all[...], dos[...], NN).astype(jnp.bfloat16)
        if len(waiting) > 0:
            finish(*waiting.pop(0))
    while waiting:
        finish(*waiting.pop(0))
    kw[...] = (dot(ds_all[...], qs[...], NN) * scale).astype(jnp.bfloat16)
    vw[...] = dv
    for b in range(subs):
        rows = slice(b * tok, (b + 1) * tok)
        dfar_ref[b, :, key_cols] = kw[rows, :]
        dfar_ref[b, :, value_cols] = vw[rows, :]
    for o, ref in enumerate(down_refs):
        ref[:, key_cols] = kw[held(o), :]
        ref[:, value_cols] = vw[held(o), :]


def attend(groups, where, base, start, queries, grads, far, own):
    tok = queries.shape[0]
    group = queries.shape[1] // HEAD_SIZE // groups
    keys = (1 + far.shape[0]) * tok
    scalar = pl.BlockSpec(memory_space=pltpu.SMEM)
    vmem = pl.BlockSpec(memory_space=pltpu.VMEM)
    wide = jax.ShapeDtypeStruct(queries.shape, jnp.bfloat16)
    rows = group * tok
    bf = lambda *shape: pltpu.VMEM(shape, jnp.bfloat16)
    return pl.pallas_call(
        functools.partial(attention_kernel, group, groups, len(own)),
        out_shape=[
            wide,
            jax.ShapeDtypeStruct((groups * group, tok), jnp.float32),
            wide,
            jax.ShapeDtypeStruct(far.shape, jnp.bfloat16),
        ]
        + [jax.ShapeDtypeStruct(x.shape, jnp.bfloat16) for x in own],
        in_specs=[scalar] * 2 + [vmem] * (4 + len(own)),
        scratch_shapes=[pltpu.VMEM((keys, tok), jnp.float32)]
        + [
            bf(rows, HEAD_SIZE),
            bf(rows, HEAD_SIZE),
            bf(keys, HEAD_SIZE),
            bf(keys, HEAD_SIZE),
            bf(HEAD_SIZE, keys),
            bf(HEAD_SIZE, keys),
            bf(keys, rows),
            bf(keys, rows),
        ]
        * groups,
        cost_estimate=pl.CostEstimate(
            flops=12 * groups * rows * keys * HEAD_SIZE,
            bytes_accessed=16 * groups * rows * HEAD_SIZE,
            transcendentals=groups * rows * keys,
        ),
        compiler_params=room(16 * groups * keys * rows),
        name="attend",
    )(where, base, start, queries, grads, far, *own)


def collect_kernel(groups, where_ref, far_ref, *refs):
    heads = far_ref.shape[1]
    own_refs, (low_ref, sum_ref) = refs[:heads], refs[heads:]
    sub, head = where_ref[1], where_ref[2]
    pieces = [(g, part) for g in range(groups) for part in range(2)]
    for o, ref in enumerate(own_refs):
        for g, part in pieces:
            at = pl.multiple_of(((head ^ o) * groups + g) * HEAD_SIZE, HEAD_SIZE)
            to = (2 * g + part) * HEAD_SIZE
            sum_ref[part, :, pl.ds(at, HEAD_SIZE)] = ref[
                :, to : to + HEAD_SIZE
            ].astype(jnp.float32)
    for h in range(heads):
        for g, part in pieces:
            at = (h * groups + g) * HEAD_SIZE
            cols = slice(at, at + HEAD_SIZE)
            to = (2 * g + part) * HEAD_SIZE
            own = sum_ref[part, :, cols]
            low = jnp.zeros_like(own)
            for s in range(far_ref.shape[0]):
                got = far_ref[s, h, :, to : to + HEAD_SIZE].astype(jnp.float32)
                own = own + jnp.where(sub < s, got, 0.0)
                low = low + jnp.where(sub < s, 0.0, got)
            sum_ref[part, :, cols] = own
            low_ref[part, :, cols] = low.astype(jnp.bfloat16)


def route_kernel(block, spots_ref, *refs):
    log_refs, outs = refs[:-2], refs[-2:]
    rows, lanes = outs[0].shape
    lane = lax.broadcasted_iota(jnp.int32, (rows, lanes), 1)
    count = len(log_refs)
    for k, out in enumerate(outs):
        owned = jnp.zeros((rows, lanes), jnp.float32)
        for d, ref in enumerate(log_refs):
            to = spots_ref[d] * block
            at = spots_ref[count * (1 + k) + d] * block
            turned = pltpu.roll(ref[...], lax.rem(to - at + lanes, lanes), 1)
            owned = jnp.where((lane >= to) & (lane < to + block), turned, owned)
        out[...] = owned


def finish_kernel(low_ref, sum_ref, mine_ref, across_ref, owned_ref, dk_ref, dv_ref):
    owned_ref[...] = mine_ref[...] + across_ref[...]
    for part, ref in enumerate((dk_ref, dv_ref)):
        ref[...] = (sum_ref[part] + low_ref[part].astype(jnp.float32)).astype(jnp.bfloat16)


def body(queries, key_rows, value_rows, grad_out, doc_ids, block_owner):
    subs = lax.axis_size("sub")
    shards = 2 * subs
    heads = lax.axis_size("head")
    half, sub, head = (lax.axis_index(name) for name in (*CTX, "head"))
    shard = half * subs + sub
    tok = queries.shape[0]
    rows = key_rows.shape[0]
    block = tok // shards
    groups = key_rows.shape[1] // HEAD_SIZE // heads
    width = 2 * groups * HEAD_SIZE
    where = jnp.stack([half, sub, head])
    vmem = pl.BlockSpec(memory_space=pltpu.VMEM)
    scalar = pl.BlockSpec(memory_space=pltpu.SMEM)

    def swap(x, axis, d):
        return lax.ppermute(x, axis, [(i, i ^ d) for i in range(lax.axis_size(axis))])

    low_keys, low_values = swap(key_rows, "half", 1), swap(value_rows, "half", 1)
    mine, *own = pl.pallas_call(
        functools.partial(own_kernel, groups),
        out_shape=[jax.ShapeDtypeStruct((heads, rows, width), jnp.bfloat16)]
        + [jax.ShapeDtypeStruct((rows, width), jnp.bfloat16)] * heads,
        in_specs=[scalar] + [vmem] * 2,
        cost_estimate=pl.CostEstimate(
            flops=1 << 21, bytes_accessed=12 * key_rows.size, transcendentals=0
        ),
        compiler_params=room(16 * key_rows.size),
        name="own",
    )(where, key_rows, value_rows)
    own = [own[0]] + [swap(own[o], "head", o) for o in range(1, heads)]
    packed = pl.pallas_call(
        functools.partial(far_kernel, groups),
        out_shape=jax.ShapeDtypeStruct((subs, heads, rows, width), jnp.bfloat16),
        in_specs=[scalar] + [vmem] * 3,
        compiler_params=room(8 * subs * rows * heads * width),
        name="far",
    )(where, mine, low_keys, low_values)
    far = lax.all_to_all(
        packed.reshape(subs * heads, rows, width), ("sub", "head"), 0, 0, tiled=True
    ).reshape(subs, tok, width)
    mine = lax.dynamic_slice_in_dim(doc_ids, shard * tok, tok)
    start = jnp.sum((doc_ids[:, None] < mine[None, :]).astype(jnp.int32), axis=0, keepdims=True)
    each = jnp.arange(subs + 1, dtype=jnp.int32)
    base = half * subs + jnp.where(each < subs, each - jnp.where(each >= sub, subs, 0), sub)
    attention, norm, dq, dfar, *down = attend(
        groups, where, base * tok, start, queries, grad_out, far, own
    )
    parts = lax.all_to_all(
        dfar.reshape(subs * heads, rows, width), ("sub", "head"), 0, 0, tiled=True
    )
    down = [down[0]] + [swap(down[o], "head", o) for o in range(1, heads)]
    logs = [norm] + [swap(norm, "sub", d) for d in range(1, subs)]
    source = half * subs + jnp.stack([sub ^ d for d in range(subs)])
    owners = jnp.stack([shard, shard + subs - 2 * subs * half])
    spots = jnp.argmax(block_owner[source][None] == owners[:, None, None], axis=2)
    spots = jnp.concatenate([source, spots.reshape(-1).astype(jnp.int32)])
    low, sums = pl.pallas_call(
        functools.partial(collect_kernel, groups),
        out_shape=[
            jax.ShapeDtypeStruct((2, *key_rows.shape), jnp.bfloat16),
            jax.ShapeDtypeStruct((2, *key_rows.shape), jnp.float32),
        ],
        in_specs=[scalar] + [vmem] * (1 + heads),
        compiler_params=room(8 * far.size),
        name="collect",
    )(where, parts.reshape(subs, heads, rows, width), *down)
    low = swap(low, "half", 1)
    routed = pl.pallas_call(
        functools.partial(route_kernel, block),
        out_shape=[jax.ShapeDtypeStruct(norm.shape, jnp.float32)] * 2,
        in_specs=[scalar] + [vmem] * subs,
        compiler_params=room(0),
        name="route",
    )(spots, *logs)
    across = swap(routed[1], "half", 1)
    owned, dk, dv = pl.pallas_call(
        finish_kernel,
        out_shape=[jax.ShapeDtypeStruct(norm.shape, jnp.float32)]
        + [jax.ShapeDtypeStruct(key_rows.shape, jnp.bfloat16)] * 2,
        compiler_params=room(32 * key_rows.size),
        name="finish",
    )(low, sums, routed[0], across)
    return (attention, owned, dq, dk, dv)


def solution(mesh):
    shards, heads = mesh.shape["ctx"], mesh.shape["head"]
    inner = Mesh(mesh.devices.reshape(2, shards // 2, heads), (*CTX, "head"))
    rows = P((*CTX, "head"), None)

    return jax.shard_map(
        body,
        mesh=inner,
        in_specs=(P(CTX, "head"), rows, rows, P(CTX, "head"), P(), P()),
        out_specs=(P(CTX, "head"), P("head", CTX), P(CTX, "head"), rows, rows),
        check_vma=False,
    )
```

```python
import functools

import jax
import jax.numpy as jnp
from jax import lax
from jax.experimental import pallas as pl
from jax.experimental.pallas import tpu as pltpu
from jax.sharding import Mesh
from jax.sharding import PartitionSpec as P

HEAD_SIZE = 128
MASK = -1e30
LOG2E = 1.4426950408889634
LN2 = 0.6931471805599453
NT = (((1,), (1,)), ((), ()))
NN = (((1,), (0,)), ((), ()))
CTX = ("half", "sub")


def dot(a, b, dims):
    return lax.dot_general(a, b, dims, preferred_element_type=jnp.float32)


def room(extra):
    return pltpu.CompilerParams(vmem_limit_bytes=min((6 << 20) + extra, 60 << 20))


def own_kernel(groups, where_ref, k_ref, v_ref, mine_ref, *own_refs):
    heads = mine_ref.shape[0]
    for g in range(groups):
        for part, ref in enumerate((k_ref, v_ref)):
            to = slice((part * groups + g) * HEAD_SIZE, (part * groups + g + 1) * HEAD_SIZE)
            for h in range(heads):
                at = (h * groups + g) * HEAD_SIZE
                mine_ref[h, :, to] = ref[:, at : at + HEAD_SIZE]
            for o, own in enumerate(own_refs):
                at = pl.multiple_of(((where_ref[2] ^ o) * groups + g) * HEAD_SIZE, HEAD_SIZE)
                own[:, to] = ref[:, pl.ds(at, HEAD_SIZE)]


def far_kernel(groups, part, where_ref, mine_ref, low_ref, *refs):
    far_hbm, far_ref, sem = refs[-3:]
    subs, heads = far_ref.shape[:2]
    cols = slice(part * groups * HEAD_SIZE, (part + 1) * groups * HEAD_SIZE)
    for h in range(heads):
        mine = mine_ref[h, :, cols]
        at = h * groups * HEAD_SIZE
        theirs = low_ref[:, at : at + groups * HEAD_SIZE]
        for dest in range(subs):
            far_ref[dest, h] = jnp.where(where_ref[1] < dest, mine, theirs)
    copy = pltpu.make_async_copy(far_ref, far_hbm.at[:, :, :, cols], sem)
    copy.start()
    copy.wait()


def attention_kernel(group, groups, heads, *refs):
    scratch = refs[-8 * groups :]
    bias, o_ref, dq_ref, dfar_ref, sems = refs[-8 * groups - 5 : -8 * groups]
    refs = list(refs[: -8 * groups - 5])
    outs = 6 + heads
    o_hbm, dq_hbm, dfar_hbm = refs[outs], refs[outs + 2], refs[outs + 3]
    refs[outs], refs[outs + 2], refs[outs + 3] = o_ref, dq_ref, dfar_ref
    copies = []

    def send(src, dst):
        copy = pltpu.make_async_copy(src, dst, sems.at[len(copies)])
        copy.start()
        copies.append(copy)

    for g in range(groups):
        wide = pl.ds(g * group * HEAD_SIZE, group * HEAD_SIZE)

        def rows_done(wide=wide):
            send(o_ref.at[:, wide], o_hbm.at[:, wide])
            send(dq_ref.at[:, wide], dq_hbm.at[:, wide])

        one_group(g, group, heads, bias, scratch[8 * g : 8 * g + 8], rows_done, *refs)
        for part in range(2):
            cols = pl.ds((part * groups + g) * HEAD_SIZE, HEAD_SIZE)
            send(dfar_ref.at[:, :, cols], dfar_hbm.at[:, :, cols])
    for copy in copies:
        copy.wait()


def one_group(
    g, group, heads, bias, scratch, rows_done, where_ref, base_ref, start_ref, q_ref, do_ref, far_ref, *refs
):
    own_refs, refs = refs[:heads], refs[heads:]
    o_ref, lse_ref, dq_ref, dfar_ref = refs[:4]
    down_refs = refs[4:]
    qs, dos, kw, vw, kt, vt, p_all, ds_all = scratch
    shift = far_ref.shape[2] // 2
    key_cols = slice(g * HEAD_SIZE, (g + 1) * HEAD_SIZE)
    value_cols = slice(shift + g * HEAD_SIZE, shift + (g + 1) * HEAD_SIZE)

    def columns(h):
        return slice((g * group + h) * HEAD_SIZE, (g * group + h + 1) * HEAD_SIZE)

    tok = q_ref.shape[0]
    scale = HEAD_SIZE ** (-0.5)
    subs = far_ref.shape[0]
    piece = tok // heads
    for h in range(group):
        qs[h * tok : (h + 1) * tok, :] = q_ref[:, columns(h)]
        dos[h * tok : (h + 1) * tok, :] = do_ref[:, columns(h)]
    for b in range(subs):
        rows = slice(b * tok, (b + 1) * tok)
        kw[rows, :] = far_ref[b, :, key_cols]
        vw[rows, :] = far_ref[b, :, value_cols]

    def held(o):
        return pl.ds(pl.multiple_of(subs * tok + (where_ref[2] ^ o) * piece, piece), piece)

    for o, ref in enumerate(own_refs):
        kw[held(o), :] = ref[:, key_cols]
        vw[held(o), :] = ref[:, value_cols]
    kt[...] = kw[...].T
    vt[...] = vw[...].T

    if g == 0:
        row = lax.broadcasted_iota(jnp.int32, (tok, tok), 0)
        query = base_ref[subs] + lax.broadcasted_iota(jnp.int32, (tok, tok), 1)
        for b in range(subs + 1):
            place = base_ref[b] + row
            allowed = (place >= start_ref[...]) & (place <= query)
            bias[b * tok : (b + 1) * tok, :] = jnp.where(allowed, 0.0, MASK)

    pair = 2
    width = pair * tok
    count = group // pair

    def at(i):
        return slice(i * width, (i + 1) * width)

    def scores(i):
        return dot(kw[...], qs[at(i), :], NT)

    def finish(i, p, inv, dp):
        low = p_all[:, at(i)]
        ot = dot(vt[...], low, NN)
        outs = [ot[:, j * tok : (j + 1) * tok].T.astype(jnp.bfloat16) for j in range(pair)]
        turned = ot.astype(jnp.bfloat16).astype(jnp.float32)
        grad = dos[at(i), :].T.astype(jnp.float32)
        delta = jnp.sum(turned * grad, axis=0, keepdims=True)
        ds_all[:, at(i)] = ((p * inv) * (dp - delta)).astype(jnp.bfloat16)
        dqt = dot(kt[...], ds_all[:, at(i)], NN) * scale
        for j in range(pair):
            h = i * pair + j
            o_ref[:, columns(h)] = outs[j]
            dq_ref[:, columns(h)] = dqt[:, j * tok : (j + 1) * tok].T.astype(jnp.bfloat16)

    following = scores(0)
    waiting = []
    for i in range(count):
        s = following
        if i + 1 < count:
            following = scores(i + 1)
        dp = dot(vw[...], dos[at(i), :], NT)
        s = s * (scale * LOG2E) + jnp.concatenate([bias[...]] * pair, axis=1)
        top = jnp.max(s, axis=0, keepdims=True)
        p = jnp.exp2(s - top)
        total = jnp.sum(p, axis=0, keepdims=True)
        inv = 1.0 / total
        lse = (top + jnp.log2(total)) * LN2
        for j in range(pair):
            h = g * group + i * pair + j
            lse_ref[h : h + 1, :] = lse[:, j * tok : (j + 1) * tok]
        p_all[:, at(i)] = (p * inv).astype(jnp.bfloat16)

        waiting.append((i, p, inv, dp))
        if i + 1 == count:
            dv = dot(p_all[...], dos[...], NN).astype(jnp.bfloat16)
        if len(waiting) > 0:
            finish(*waiting.pop(0))
    while waiting:
        finish(*waiting.pop(0))
    rows_done()
    kw[...] = (dot(ds_all[...], qs[...], NN) * scale).astype(jnp.bfloat16)
    vw[...] = dv
    for b in range(subs):
        rows = slice(b * tok, (b + 1) * tok)
        dfar_ref[b, :, key_cols] = kw[rows, :]
        dfar_ref[b, :, value_cols] = vw[rows, :]
    for o, ref in enumerate(down_refs):
        ref[:, key_cols] = kw[held(o), :]
        ref[:, value_cols] = vw[held(o), :]


def attend(groups, where, base, start, queries, grads, far, own):
    tok = queries.shape[0]
    group = queries.shape[1] // HEAD_SIZE // groups
    keys = (1 + far.shape[0]) * tok
    scalar = pl.BlockSpec(memory_space=pltpu.SMEM)
    vmem = pl.BlockSpec(memory_space=pltpu.VMEM)
    hbm = pl.BlockSpec(memory_space=pl.ANY)
    wide = jax.ShapeDtypeStruct(queries.shape, jnp.bfloat16)
    rows = group * tok
    bf = lambda *shape: pltpu.VMEM(shape, jnp.bfloat16)
    return pl.pallas_call(
        functools.partial(attention_kernel, group, groups, len(own)),
        out_shape=[
            wide,
            jax.ShapeDtypeStruct((groups * group, tok), jnp.float32),
            wide,
            jax.ShapeDtypeStruct(far.shape, jnp.bfloat16),
        ]
        + [jax.ShapeDtypeStruct(x.shape, jnp.bfloat16) for x in own],
        in_specs=[scalar] * 2 + [vmem] * (4 + len(own)),
        out_specs=[hbm, vmem, hbm, hbm] + [vmem] * len(own),
        scratch_shapes=[
            pltpu.VMEM((keys, tok), jnp.float32),
            bf(*queries.shape),
            bf(*queries.shape),
            bf(*far.shape),
            pltpu.SemaphoreType.DMA((4 * groups,)),
        ]
        + [
            bf(rows, HEAD_SIZE),
            bf(rows, HEAD_SIZE),
            bf(keys, HEAD_SIZE),
            bf(keys, HEAD_SIZE),
            bf(HEAD_SIZE, keys),
            bf(HEAD_SIZE, keys),
            bf(keys, rows),
            bf(keys, rows),
        ]
        * groups,
        cost_estimate=pl.CostEstimate(
            flops=12 * groups * rows * keys * HEAD_SIZE,
            bytes_accessed=16 * groups * rows * HEAD_SIZE,
            transcendentals=groups * rows * keys,
        ),
        compiler_params=room(16 * groups * keys * rows),
        name="attend",
    )(where, base, start, queries, grads, far, *own)


def collect_kernel(groups, where_ref, far_ref, *refs):
    heads = far_ref.shape[1]
    own_refs, (low_ref, sum_ref) = refs[:heads], refs[heads:]
    sub, head = where_ref[1], where_ref[2]
    pieces = [(g, part) for g in range(groups) for part in range(2)]
    for o, ref in enumerate(own_refs):
        for g, part in pieces:
            at = pl.multiple_of(((head ^ o) * groups + g) * HEAD_SIZE, HEAD_SIZE)
            to = (part * groups + g) * HEAD_SIZE
            sum_ref[part, :, pl.ds(at, HEAD_SIZE)] = ref[
                :, to : to + HEAD_SIZE
            ].astype(jnp.float32)
    for h in range(heads):
        for g, part in pieces:
            at = (h * groups + g) * HEAD_SIZE
            cols = slice(at, at + HEAD_SIZE)
            to = (part * groups + g) * HEAD_SIZE
            own = sum_ref[part, :, cols]
            low = jnp.zeros_like(own)
            for s in range(far_ref.shape[0]):
                got = far_ref[s, h, :, to : to + HEAD_SIZE].astype(jnp.float32)
                own = own + jnp.where(sub < s, got, 0.0)
                low = low + jnp.where(sub < s, 0.0, got)
            sum_ref[part, :, cols] = own
            low_ref[part, :, cols] = low.astype(jnp.bfloat16)


def route_kernel(block, spots_ref, *refs):
    log_refs, outs = refs[:-2], refs[-2:]
    rows, lanes = outs[0].shape
    lane = lax.broadcasted_iota(jnp.int32, (rows, lanes), 1)
    count = len(log_refs)
    for k, out in enumerate(outs):
        owned = jnp.zeros((rows, lanes), jnp.float32)
        for d, ref in enumerate(log_refs):
            to = spots_ref[d] * block
            at = spots_ref[count * (1 + k) + d] * block
            turned = pltpu.roll(ref[...], lax.rem(to - at + lanes, lanes), 1)
            owned = jnp.where((lane >= to) & (lane < to + block), turned, owned)
        out[...] = owned


def finish_kernel(low_ref, sum_ref, mine_ref, across_ref, owned_ref, dk_ref, dv_ref):
    owned_ref[...] = mine_ref[...] + across_ref[...]
    for part, ref in enumerate((dk_ref, dv_ref)):
        ref[...] = (sum_ref[part] + low_ref[part].astype(jnp.float32)).astype(jnp.bfloat16)


def body(queries, key_rows, value_rows, grad_out, doc_ids, block_owner):
    subs = lax.axis_size("sub")
    shards = 2 * subs
    heads = lax.axis_size("head")
    half, sub, head = (lax.axis_index(name) for name in (*CTX, "head"))
    shard = half * subs + sub
    tok = queries.shape[0]
    rows = key_rows.shape[0]
    block = tok // shards
    groups = key_rows.shape[1] // HEAD_SIZE // heads
    width = 2 * groups * HEAD_SIZE
    where = jnp.stack([half, sub, head])
    vmem = pl.BlockSpec(memory_space=pltpu.VMEM)
    scalar = pl.BlockSpec(memory_space=pltpu.SMEM)

    def swap(x, axis, d):
        return lax.ppermute(x, axis, [(i, i ^ d) for i in range(lax.axis_size(axis))])

    low_keys, low_values = swap(key_rows, "half", 1), swap(value_rows, "half", 1)
    mine, *own = pl.pallas_call(
        functools.partial(own_kernel, groups),
        out_shape=[jax.ShapeDtypeStruct((heads, rows, width), jnp.bfloat16)]
        + [jax.ShapeDtypeStruct((rows, width), jnp.bfloat16)] * heads,
        in_specs=[scalar] + [vmem] * 2,
        cost_estimate=pl.CostEstimate(
            flops=1 << 21, bytes_accessed=12 * key_rows.size, transcendentals=0
        ),
        compiler_params=room(16 * key_rows.size),
        name="own",
    )(where, key_rows, value_rows)
    own = [own[0]] + [swap(own[o], "head", o) for o in range(1, heads)]
    packed = []
    anywhere = pl.BlockSpec(memory_space=pl.ANY)
    for part, low in enumerate((low_keys, low_values)):
        packed = [
            pl.pallas_call(
                functools.partial(far_kernel, groups, part),
                out_shape=jax.ShapeDtypeStruct((subs, heads, rows, width), jnp.bfloat16),
                in_specs=[scalar] + [vmem] * 2 + [anywhere] * len(packed),
                out_specs=anywhere,
                scratch_shapes=[
                    pltpu.VMEM((subs, heads, rows, width // 2), jnp.bfloat16),
                    pltpu.SemaphoreType.DMA,
                ],
                input_output_aliases={3: 0} if packed else {},
                compiler_params=room(8 * subs * rows * heads * width),
                name="far",
            )(where, mine, low, *packed)
        ]
    far = lax.all_to_all(
        packed[0].reshape(subs * heads, rows, width), ("sub", "head"), 0, 0, tiled=True
    ).reshape(subs, tok, width)
    mine = lax.dynamic_slice_in_dim(doc_ids, shard * tok, tok)
    start = jnp.sum((doc_ids[:, None] < mine[None, :]).astype(jnp.int32), axis=0, keepdims=True)
    each = jnp.arange(subs + 1, dtype=jnp.int32)
    base = half * subs + jnp.where(each < subs, each - jnp.where(each >= sub, subs, 0), sub)
    attention, norm, dq, dfar, *down = attend(
        groups, where, base * tok, start, queries, grad_out, far, own
    )
    parts = lax.all_to_all(
        dfar.reshape(subs * heads, rows, width), ("sub", "head"), 0, 0, tiled=True
    )
    down = [down[0]] + [swap(down[o], "head", o) for o in range(1, heads)]
    logs = [norm] + [swap(norm, "sub", d) for d in range(1, subs)]
    source = half * subs + jnp.stack([sub ^ d for d in range(subs)])
    owners = jnp.stack([shard, shard + subs - 2 * subs * half])
    spots = jnp.argmax(block_owner[source][None] == owners[:, None, None], axis=2)
    spots = jnp.concatenate([source, spots.reshape(-1).astype(jnp.int32)])
    low, sums = pl.pallas_call(
        functools.partial(collect_kernel, groups),
        out_shape=[
            jax.ShapeDtypeStruct((2, *key_rows.shape), jnp.bfloat16),
            jax.ShapeDtypeStruct((2, *key_rows.shape), jnp.float32),
        ],
        in_specs=[scalar] + [vmem] * (1 + heads),
        compiler_params=room(8 * far.size),
        name="collect",
    )(where, parts.reshape(subs, heads, rows, width), *down)
    low = swap(low, "half", 1)
    routed = pl.pallas_call(
        functools.partial(route_kernel, block),
        out_shape=[jax.ShapeDtypeStruct(norm.shape, jnp.float32)] * 2,
        in_specs=[scalar] + [vmem] * subs,
        compiler_params=room(0),
        name="route",
    )(spots, *logs)
    across = swap(routed[1], "half", 1)
    owned, dk, dv = pl.pallas_call(
        finish_kernel,
        out_shape=[jax.ShapeDtypeStruct(norm.shape, jnp.float32)]
        + [jax.ShapeDtypeStruct(key_rows.shape, jnp.bfloat16)] * 2,
        compiler_params=room(32 * key_rows.size),
        name="finish",
    )(low, sums, routed[0], across)
    return (attention, owned, dq, dk, dv)


def solution(mesh):
    shards, heads = mesh.shape["ctx"], mesh.shape["head"]
    inner = Mesh(mesh.devices.reshape(2, shards // 2, heads), (*CTX, "head"))
    rows = P((*CTX, "head"), None)

    return jax.shard_map(
        body,
        mesh=inner,
        in_specs=(P(CTX, "head"), rows, rows, P(CTX, "head"), P(), P()),
        out_specs=(P(CTX, "head"), P("head", CTX), P(CTX, "head"), rows, rows),
        check_vma=False,
    )
```
